32 devices in a mesh: grp: 2 (over y), ctx: 4 (over z), hd: 4 (over x, core).
Axes of the slice: x: 2, y: 2, z: 4, core: 2. Of those that a mesh axis runs over, the one named last changes fastest.
Arguments:
- query: bfloat16 [1024, 4096], P(('grp', 'ctx'), 'hd'), parts along dimension 0, may hold values from -6 to 6
- keys: bfloat16 [1024, 1024], P(('grp', 'ctx'), 'hd'), parts along dimension 0, may hold values from -6 to 6
- values: bfloat16 [1024, 1024], P(('grp', 'ctx'), 'hd'), parts along dimension 0, may hold values from -6 to 6
- m_x: bfloat16 [1024, 8192], P(('grp', 'ctx'), 'hd'), parts along dimension 0, may hold values from -6 to 6
- m_z: bfloat16 [1024, 8192], P(('grp', 'ctx'), 'hd'), parts along dimension 0, may hold values from -6 to 6
- m_b: bfloat16 [1024, 1024], P(('grp', 'ctx'), 'hd'), parts along dimension 0, may hold values from -6 to 6
- m_c: bfloat16 [1024, 1024], P(('grp', 'ctx'), 'hd'), parts along dimension 0, may hold values from -0.5 to 0.5
- dt_raw: bfloat16 [1024, 128], P(('grp', 'ctx'), 'hd'), parts along dimension 0, may hold values from -5 to 25
- dt_bias: float32 [128], P('hd'), may hold values from -0.5 to 0.5
- a_log: float32 [128], P('hd'), may hold values from -10 to 0
- d_skip: float32 [128], P('hd'), may hold values from 0.5 to 2
- norm_gain: float32 [8192], P('hd'), may hold values from 0.5 to 1.5
Outputs:
- context: bfloat16 [1024, 4096], P(('grp', 'ctx'), 'hd'), parts along dimension 0
- mixed: bfloat16 [1024, 8192], P(('grp', 'ctx'), 'hd'), parts along dimension 0
The draws below stay inside these ranges and needn't reach their ends.
There are 2 independent parts, one for each index of `grp`. The reference program is written for one: setup_inputs(seed, part) draws one part's arguments, and reference() takes and returns one part's arrays. A program takes and returns all parts, laid end to end along the dimension named above; an argument that names none is the same for every part. Nothing has to cross between parts.
All inputs are finite; a program needn't handle non-finite values.
Results may differ from the reference program's by a relative error of at most 0.009.
Values may be sent and summed in bfloat16 or wider, within the bound.
A program may use at most 64 MiB of HBM per device.

```python
import math
import jax
import jax.numpy as jnp
from jax import lax

QUERY_HEADS = 32
KEY_VALUE_HEADS = 8
HEAD_SIZE = 128
MH = 128
MP = 64
MN = 128
MG = 8
TOK_DEV = 128
SEQUENCE_TOKENS = 512
N_CTX = 4


def spike_rows(key):
    return jax.random.randint(jax.random.fold_in(key, 101), (2,), 0, SEQUENCE_TOKENS)


def spike_level():
    return min(SEQUENCE_TOKENS // 20, 256)


def draw_keys(key, part):
    random_seed_key = jax.random.fold_in(key, 606)
    sampled = jnp.clip(jax.random.normal(random_seed_key, (SEQUENCE_TOKENS, KEY_VALUE_HEADS * HEAD_SIZE), jnp.float32), -6.0, 6.0)
    return sampled.astype(jnp.bfloat16)


def draw_query(key, part):
    random_seed_key = jax.random.fold_in(key, 707)
    sampled = jnp.clip(jax.random.normal(random_seed_key, (SEQUENCE_TOKENS, QUERY_HEADS * HEAD_SIZE), jnp.float32), -6.0, 6.0)
    return sampled.astype(jnp.bfloat16)


def draw_m_x(key, part):
    selected = spike_rows(key)
    first_key = jax.random.fold_in(jax.random.fold_in(key, 303), 0)
    sampled = jax.random.normal(first_key, (SEQUENCE_TOKENS, MH * MP), jnp.float32)
    sampled = jnp.clip(sampled, -6.0, 6.0)
    flagged = jnp.any(jnp.arange(SEQUENCE_TOKENS)[:, None] == selected[None, :], axis=1)
    sampled = jnp.where(flagged[:, None], sampled * (0.06 / spike_level()), sampled)
    return sampled.astype(jnp.bfloat16)


def draw_dt_raw(key, part):
    selected = spike_rows(key)
    first_key, other_random_key = jax.random.split(jax.random.fold_in(key, 202))
    rough = jax.random.uniform(first_key, (SEQUENCE_TOKENS, MH), jnp.float32, -1.0, 1.0) - 3.0
    offsets = jax.random.uniform(other_random_key, (SEQUENCE_TOKENS // TOK_DEV, 1), jnp.float32, -0.7, 0.7)
    sampled = rough + jnp.repeat(offsets, TOK_DEV, axis=0)
    flagged = jnp.any(jnp.arange(SEQUENCE_TOKENS)[:, None] == selected[None, :], axis=1)
    sampled = jnp.where(flagged[:, None], jnp.float32(spike_level()), sampled)
    return sampled.astype(jnp.bfloat16)


def draw_a_log(key, part):
    first_key, other_random_key, third_key = jax.random.split(jax.random.fold_in(key, 404), 3)
    quick = jax.random.bernoulli(first_key, 0.5, (MH,))
    window = jax.random.uniform(other_random_key, (MH,), jnp.float32, 20.0, 60.0)
    slack = jax.random.uniform(third_key, (MH,), jnp.float32, 0.3, 1.0)
    fast_rate = -jnp.log(0.06 * window)
    slow_rate = -jnp.log(0.06 * SEQUENCE_TOKENS) - slack
    return jnp.where(quick, fast_rate, slow_rate).astype(jnp.float32)


def block_levels(rng, shape, cuts, least, top_value):
    level = 1.0
    for position, blocks in cuts:
        steps = jax.random.uniform(jax.random.fold_in(jax.random.fold_in(rng, 6), position), (blocks,), jnp.float32, least / len(cuts), top_value / len(cuts))
        level = level * jnp.repeat(jnp.exp(steps), shape[position] // blocks).reshape((-1,) + (1,) * (len(shape) - 1 - position))
    return level


def noise(own_key, extent, scale, bound, shards=(), kind=jnp.bfloat16):
    level = block_levels(own_key, extent, shards, -0.22, 0.18) if shards else 1.0
    values = jax.random.normal(own_key, extent, jnp.float32) * scale * level
    return jnp.minimum(jnp.maximum(values, -bound), bound).astype(kind)


def setup_inputs(seed: int = 0, part: int = 0) -> dict:
    streams_of = jax.random.split(jax.random.key(seed), 13)
    part_keys = jax.random.split(jax.random.fold_in(streams_of[12], part), 13)
    return {
        "query": draw_query(jax.random.fold_in(jax.random.fold_in(streams_of[12], part), 71), part),
        "keys": draw_keys(jax.random.fold_in(jax.random.fold_in(streams_of[12], part), 71), part),
        "values": noise(part_keys[2], (SEQUENCE_TOKENS, KEY_VALUE_HEADS * HEAD_SIZE), 1.0, 6.0, ((0, 4), (1, 4))),
        "m_x": draw_m_x(jax.random.fold_in(jax.random.fold_in(streams_of[12], part), 71), part),
        "m_z": noise(part_keys[4], (SEQUENCE_TOKENS, MH * MP), 1.0, 6.0, ((0, 4), (1, 4))),
        "m_b": noise(part_keys[5], (SEQUENCE_TOKENS, MG * MN), 1.0, 6.0, ((0, 4), (1, 4))),
        "m_c": noise(part_keys[6], (SEQUENCE_TOKENS, MG * MN), MN ** -0.5, 0.5, ((0, 4), (1, 4))),
        "dt_raw": draw_dt_raw(jax.random.fold_in(jax.random.fold_in(streams_of[12], part), 71), part),
        "dt_bias": jnp.clip(jax.random.uniform(streams_of[8], (MH,), jnp.float32, -0.5, 0.5) * block_levels(streams_of[8], (MH,), ((0, 4),), -0.4, 0.0), -0.5, 0.5),
        "a_log": draw_a_log(jax.random.fold_in(streams_of[12], 71), part),
        "d_skip": jnp.clip(0.5 + 1.5 * jax.random.uniform(streams_of[10], (MH,), jnp.float32) ** block_levels(streams_of[10], (MH,), ((0, 4),), -0.2, 0.2), 0.5, 2.0),
        "norm_gain": jnp.clip(1.0 + 0.1 * jax.random.normal(streams_of[11], (MH * MP,), jnp.float32), 0.5, 1.5),
    }


highest = lax.Precision.HIGHEST
norm_eps = 1e-05

def folded_to_sequence(whole):
    half_rows = whole.shape[0] // (2 * N_CTX)
    blocks = whole.reshape((N_CTX, 2, half_rows) + whole.shape[1:])
    return jnp.concatenate([blocks[:, 0], blocks[::-1, 1]], axis=0).reshape(whole.shape)

def attention(query, keys, values):
    sequence_length = query.shape[0]
    heads_per_group = QUERY_HEADS // KEY_VALUE_HEADS
    every_query = query.astype(jnp.float32).reshape(sequence_length, KEY_VALUE_HEADS, heads_per_group, HEAD_SIZE)
    every_key = keys.astype(jnp.float32).reshape(sequence_length, KEY_VALUE_HEADS, HEAD_SIZE)
    every_value = values.astype(jnp.float32).reshape(sequence_length, KEY_VALUE_HEADS, HEAD_SIZE)
    rows_per_block = math.gcd(sequence_length, 256)
    query_block_list = every_query.reshape(sequence_length // rows_per_block, rows_per_block, KEY_VALUE_HEADS, heads_per_group, HEAD_SIZE)
    key_pos = jnp.arange(sequence_length, dtype=jnp.int32)

    def query_block(packed):
        block_query, block_index = packed
        query_pos = block_index * rows_per_block + jnp.arange(rows_per_block, dtype=jnp.int32)
        scores = jnp.einsum('qhgd,khd->hgqk', block_query, every_key, precision=highest) / math.sqrt(HEAD_SIZE)
        visible = key_pos[None, :] <= query_pos[:, None]
        scores = jnp.where(visible, scores, -jnp.inf)
        largest = lax.optimization_barrier(jnp.max(scores, axis=-1, keepdims=True))
        expons = jnp.exp(scores - largest)
        totals = lax.optimization_barrier(jnp.sum(expons, axis=-1))
        rounded = lax.optimization_barrier(expons.astype(jnp.bfloat16)).astype(jnp.float32)
        summed = jnp.einsum('hgqk,khd->qhgd', rounded, every_value, precision=highest)
        return (summed / jnp.transpose(totals, (2, 0, 1))[..., None]).reshape(rows_per_block, QUERY_HEADS * HEAD_SIZE)
    result = lax.map(query_block, (query_block_list, jnp.arange(sequence_length // rows_per_block, dtype=jnp.int32)))
    return result.reshape(sequence_length, QUERY_HEADS * HEAD_SIZE).astype(jnp.bfloat16)

def ssd_block(inputs, steps, rates, b_rows, c_rows):
    intersection = jnp.dot(c_rows, b_rows.T, preferred_element_type=jnp.float32)
    inputs = inputs.astype(jnp.float32)
    b_rows = b_rows.astype(jnp.float32)
    sequence_length = inputs.shape[0]
    running = jnp.cumsum(-steps * rates, axis=0)
    lower = jnp.arange(sequence_length)[:, None] >= jnp.arange(sequence_length)[None, :]
    spread = running[:, None, :] - running[None, :, :]
    decay = jnp.exp(jnp.where(lower[:, :, None], spread, -jnp.inf))
    weights = intersection[:, :, None] * decay * steps[None, :, :]
    inner = jnp.einsum('ijh,jhp->ihp', weights, inputs, precision=highest)
    tail_weight = jnp.exp(running[-1][None, :] - running) * steps
    state = jnp.einsum('jh,jhp,jn->hpn', tail_weight, inputs, b_rows, precision=highest)
    return (inner, state, jnp.exp(running[-1]), jnp.exp(running))

def chain_states(earlier, later):
    return (earlier[0] * later[0], earlier[1] * later[0][..., None, None] + later[1])

def ssd_sequence(inputs, steps, rates, b_rows, c_rows):
    sequence_length, head_count, width = inputs.shape
    block_len = math.gcd(sequence_length, 128)
    count = sequence_length // block_len
    c_blocks = c_rows.reshape(count, block_len, -1)
    inner, state, totals, scaled = jax.vmap(ssd_block, in_axes=(0, 0, None, 0, 0))(inputs.reshape(count, block_len, head_count, width), steps.reshape(count, block_len, head_count), rates, b_rows.reshape(count, block_len, -1), c_blocks)
    running = lax.associative_scan(chain_states, (totals, state))
    entering = jnp.concatenate([jnp.zeros_like(running[1][:1]), running[1][:-1]], axis=0)
    carried = jnp.einsum('cqn,chpn->cqhp', c_blocks.astype(jnp.float32), entering, precision=highest) * scaled[..., None]
    return (inner + carried).reshape(sequence_length, head_count, width)

def gated_norm(gated_rows, norm_scale, group_count):
    row_count = gated_rows.shape[0]
    widened = lax.optimization_barrier(gated_rows).astype(jnp.float32).reshape(row_count, group_count, -1)
    power = lax.optimization_barrier(jnp.mean(widened * widened, axis=-1, keepdims=True))
    return ((widened * lax.rsqrt(power + norm_eps)).reshape(row_count, -1) * norm_scale).astype(jnp.bfloat16)

def mamba(m_x, m_z, m_b, m_c, dt_raw, dt_bias, a_log, d_skip, norm_gain):
    sequence_length = m_x.shape[0]
    per_group = MH // MG
    x_all = m_x.reshape(sequence_length, MG, per_group, MP)
    step_all = jax.nn.softplus(dt_raw.astype(jnp.float32) + dt_bias).reshape(sequence_length, MG, per_group)
    rates = jnp.exp(a_log).reshape(MG, per_group)
    b_all = m_b.reshape(sequence_length, MG, MN)
    c_all = m_c.reshape(sequence_length, MG, MN)

    def by_group(packed):
        return ssd_sequence(packed[0], packed[1], packed[2], packed[3], packed[4])
    outputs = lax.map(by_group, (jnp.transpose(x_all, (1, 0, 2, 3)), jnp.transpose(step_all, (1, 0, 2)), rates, jnp.transpose(b_all, (1, 0, 2)), jnp.transpose(c_all, (1, 0, 2))))
    outputs = jnp.transpose(outputs, (1, 0, 2, 3)) + d_skip.reshape(MG, per_group)[None, :, :, None] * x_all.astype(jnp.float32)
    gated = (outputs.reshape(sequence_length, MH * MP) * jax.nn.silu(m_z.astype(jnp.float32))).astype(jnp.bfloat16)
    return gated_norm(gated, norm_gain, MG)

def reference(query, keys, values, m_x, m_z, m_b, m_c, dt_raw, dt_bias, a_log, d_skip, norm_gain):
    context = attention(folded_to_sequence(query), folded_to_sequence(keys), folded_to_sequence(values))
    mixed = mamba(folded_to_sequence(m_x), folded_to_sequence(m_z), folded_to_sequence(m_b), folded_to_sequence(m_c), folded_to_sequence(dt_raw), dt_bias, a_log, d_skip, norm_gain)
    return (context, mixed)
```

```python
import functools
import math

import jax
import jax.numpy as jnp
from jax import lax
from jax.experimental import pallas as pl
from jax.experimental.pallas import tpu as pltpu
from jax.sharding import PartitionSpec as P

HEAD_SIZE = 128
MP = 64
MN = 128
NORM_EPS = 1e-05
MASKED = -1e30
HIGHEST = lax.Precision.HIGHEST
F32 = jnp.float32
BF16 = jnp.bfloat16


def dot(a, b, ca=1, cb=0, precision=None):
    return lax.dot_general(
        a, b, (((ca,), (cb,)), ((), ())), preferred_element_type=F32, precision=precision
    )


def kernel(
    n, q_ref, k_ref, v_ref, x_ref, z_ref, b_ref, c_ref, dt_ref, bias_ref, alog_ref, skip_ref,
    gain_ref, ctx_out, mix_out,
    k_all, v_all, bias_scr, ctx_stage, mix_stage, gated, base_scr, er_scr, hs, runt, gmask,
    buf_a, buf_b, out_a, out_b, sloc_b, tot_b,
    k_send, k_recv, v_send, v_recv, a_send, a_recv, b_send, b_recv, o_send, o_recv,
):
    me = lax.axis_index("ctx")
    tok = q_ref.shape[0]
    half = tok // 2
    heads = dt_ref.shape[1]
    width = x_ref.shape[1]
    groups = b_ref.shape[1] // MN
    group_width = width // groups
    pieces, _, piece = buf_a.shape
    per_piece = piece // MP
    per_group = group_width // piece
    q_heads = q_ref.shape[1] // HEAD_SIZE
    repeat = q_ref.shape[1] // k_ref.shape[1]
    mesh_id = pl.DeviceIdType.MESH

    barrier = pltpu.get_barrier_semaphore()

    def greet(d, _):
        peer = lax.rem(me + d, n)
        pl.semaphore_signal(barrier, inc=1, device_id={"ctx": peer}, device_id_type=mesh_id)
        return 0

    lax.fori_loop(1, n, greet, 0)
    pl.semaphore_wait(barrier, n - 1)

    def remote(src, dst, send, recv, peer):
        return pltpu.make_async_remote_copy(
            src_ref=src, dst_ref=dst, send_sem=send, recv_sem=recv,
            device_id={"ctx": peer}, device_id_type=mesh_id,
        )

    def kv_copies(slot, sem_slot, peer, rows):
        return (
            remote(k_ref.at[rows], k_all.at[slot, rows], k_send.at[sem_slot], k_recv.at[slot], peer),
            remote(v_ref.at[rows], v_all.at[slot, rows], v_send.at[sem_slot], v_recv.at[slot], peer),
        )

    first = pl.ds(0, half)
    both = pl.ds(0, tok)

    def start_kv(d, _):
        @pl.when(me + d < n)
        def _():
            for copy in kv_copies(me, me + d, me + d, first):
                copy.start()

        @pl.when(me - d >= 0)
        def _():
            for copy in kv_copies(me, me - d, me - d, both):
                copy.start()

        return 0

    lax.fori_loop(1, n, start_kv, 0)

    raw = dt_ref[...].astype(F32) + bias_ref[...]
    steps = jnp.maximum(raw, 0.0) + jnp.log1p(jnp.exp(-jnp.abs(raw)))
    decay = -steps * jnp.exp(alog_ref[...])
    row = lax.broadcasted_iota(jnp.int32, (tok, tok), 0)
    col = lax.broadcasted_iota(jnp.int32, (tok, tok), 1)
    lower = (col <= row) & ((row < half) == (col < half))
    tri = lower.astype(F32)
    hs[0:tok, :] = dot(tri, decay, precision=HIGHEST)
    hs[tok : 2 * tok, :] = steps
    hs[2 * tok :, :] = jnp.broadcast_to(skip_ref[...], (8, heads))
    runt[...] = dot(decay, tri, 0, 1, precision=HIGHEST)
    for g in range(groups):
        cols = slice(g * MN, (g + 1) * MN)
        gmask[g] = jnp.where(lower, dot(c_ref[:, cols], b_ref[:, cols], 1, 1), 0.0)

    @pl.when(me == 0)
    def _():
        buf_a[...] = jnp.zeros_like(buf_a)

    lane_head = lax.broadcasted_iota(jnp.int32, (heads, piece), 1) // MP
    head_row = lax.broadcasted_iota(jnp.int32, (heads, piece), 0)
    wide_head = lax.broadcasted_iota(jnp.int32, (heads, per_piece * tok), 1) // tok
    wide_row = lax.broadcasted_iota(jnp.int32, (heads, per_piece * tok), 0)
    left = lax.broadcasted_iota(jnp.int32, (tok, 2 * MP), 1) < MP

    def place(src, dst_of, kind, block_id, which):
        owner = block_id // 2
        slot = lax.rem(block_id, 2)

        @pl.when(owner == me)
        def _():
            pltpu.make_async_copy(src, dst_of(slot), o_recv.at[kind, slot]).start()

        @pl.when(owner != me)
        def _():
            remote(src, dst_of(slot), o_send.at[kind, which], o_recv.at[kind, slot], owner).start()

    def block_id(which):
        return me if which == 0 else 2 * n - 1 - me

    def finish_group(k, which):
        @pl.when(lax.rem(k + 1, per_group) == 0)
        def _():
            g = k // per_group
            cols = pl.ds(pl.multiple_of(g * group_width, group_width), group_width)
            rows = pl.ds(which * half, half)
            value = gated[rows, cols].astype(F32)
            power = jnp.mean(value * value, axis=-1, keepdims=True)
            mix_stage[rows, cols] = (value * lax.rsqrt(power + NORM_EPS) * gain_ref[:, cols]).astype(BF16)
            place(
                mix_stage.at[rows, cols],
                lambda slot: mix_out.at[pl.ds(pl.multiple_of(slot * half, half), half), cols],
                g, block_id(which), which,
            )

    def silu(value):
        return value / (1.0 + jnp.exp(-value))

    def step_a(k):
        cols = pl.ds(pl.multiple_of(k * piece, piece), piece)
        g = k // per_group
        gcols = pl.ds(pl.multiple_of(g * MN, MN), MN)
        pick = (head_row == k * per_piece + lane_head).astype(F32)
        spread = dot(hs[...], pick, precision=HIGHEST)
        run, step, skip = spread[0:tok], spread[tok : 2 * tok], spread[2 * tok : 2 * tok + 1]
        xs = x_ref[:, cols].astype(F32)
        xdt = xs * step
        last_a, last_b = run[half - 1 : half], run[tok - 1 : tok]
        b_rows = b_ref[:, gcols]
        add_a = dot(b_rows[0:half], (xdt[0:half] * jnp.exp(last_a - run[0:half])).astype(BF16), 0, 0)
        sloc_b[k] = dot(b_rows[half:], (xdt[half:] * jnp.exp(last_b - run[half:])).astype(BF16), 0, 0)
        tot_b[k] = jnp.broadcast_to(jnp.exp(last_b), (8, piece))
        er = jnp.exp(run)
        er_scr[:, cols] = er[half:]

        @pl.when(me > 0)
        def _():
            remote(out_a.at[k], buf_a.at[k], a_send.at[k], a_recv.at[k], me).wait_recv()

        state = (buf_a[k].astype(F32) * jnp.exp(last_a) + add_a).astype(BF16)

        @pl.when(me < n - 1)
        def _():
            out_a[k] = state
            remote(out_a.at[k], buf_a.at[k], a_send.at[k], a_recv.at[k], me + 1).start()

        @pl.when(me == n - 1)
        def _():
            buf_b[k] = state

        wide = dot(hs[0:tok, :], (wide_row == k * per_piece + wide_head).astype(F32), precision=HIGHEST)
        gm = gmask[g]
        inner = []
        for pair in range(per_piece // 2):
            weights = []
            for which in range(2):
                h = 2 * pair + which
                gap = wide[:, h * tok : (h + 1) * tok] - runt[pl.ds(k * per_piece + h, 1), :]
                weights.append((jnp.exp(jnp.minimum(gap, 0.0)) * gm).astype(BF16))
            part = xdt[:, pair * 2 * MP : (pair + 1) * 2 * MP]
            stacked = jnp.concatenate(
                [jnp.where(left, part, 0.0).astype(BF16), jnp.where(left, 0.0, part).astype(BF16)], axis=0
            )
            inner.append(dot(jnp.concatenate(weights, axis=1), stacked))
        base = jnp.concatenate(inner, axis=1) + skip * xs
        base_scr[:, cols] = base[half:]
        carried = dot(c_ref[0:half, gcols], buf_a[k]) * er[0:half]
        z = z_ref[0:half, cols].astype(F32)
        gated[0:half, cols] = ((base[0:half] + carried) * silu(z)).astype(BF16)
        finish_group(k, 0)

    def step_b(k):
        cols = pl.ds(pl.multiple_of(k * piece, piece), piece)
        gcols = pl.ds(pl.multiple_of((k // per_group) * MN, MN), MN)

        @pl.when(me < n - 1)
        def _():
            remote(out_b.at[k], buf_b.at[k], b_send.at[k], b_recv.at[k], me).wait_recv()

        @pl.when(me > 0)
        def _():
            out_b[k] = (buf_b[k].astype(F32) * tot_b[k][0:1] + sloc_b[k]).astype(BF16)
            remote(out_b.at[k], buf_b.at[k], b_send.at[k], b_recv.at[k], me - 1).start()

        carried = dot(c_ref[half:, gcols], buf_b[k]) * er_scr[:, cols]
        z = z_ref[half:, cols].astype(F32)
        gated[half:, cols] = ((base_scr[:, cols] + carried) * silu(z)).astype(BF16)
        finish_group(k, 1)

    def attention():
        def wait_kv(s, _):
            @pl.when(s < me)
            def _():
                for copy in kv_copies(s, s, me, first):
                    copy.wait_recv()
                k_all[s, half:, :] = jnp.zeros((half, k_ref.shape[1]), BF16)
                v_all[s, half:, :] = jnp.zeros((half, k_ref.shape[1]), BF16)

            @pl.when(s > me)
            def _():
                for copy in kv_copies(s, s, me, both):
                    copy.wait_recv()

            return 0

        lax.fori_loop(0, n, wait_kv, 0)
        k_all[me] = k_ref[...]
        v_all[me] = v_ref[...]
        key = lax.broadcasted_iota(jnp.int32, (tok, n * tok), 1)
        source = key // tok
        within = key - source * tok
        key_pos = jnp.where(
            within < half, source * half + within, (2 * n - 2 - source) * half + within
        )
        query = lax.broadcasted_iota(jnp.int32, (tok, n * tok), 0)
        query_pos = jnp.where(query < half, me * half + query, (2 * n - 2 - me) * half + query)
        bias_scr[...] = jnp.where(key_pos <= query_pos, 0.0, MASKED)
        scale = 1.0 / math.sqrt(HEAD_SIZE)

        def one_head(h, _):
            hcols = pl.ds(pl.multiple_of(h * HEAD_SIZE, HEAD_SIZE), HEAD_SIZE)
            kcols = pl.ds(pl.multiple_of((h // repeat) * HEAD_SIZE, HEAD_SIZE), HEAD_SIZE)
            keys = k_all[:, :, kcols].reshape(n * tok, HEAD_SIZE)
            values = v_all[:, :, kcols].reshape(n * tok, HEAD_SIZE)
            scores = dot(q_ref[:, hcols], keys, 1, 1) * scale + bias_scr[...]
            expo = jnp.exp(scores - jnp.max(scores, axis=-1, keepdims=True))
            total = jnp.sum(expo, axis=-1, keepdims=True)
            ctx_stage[:, hcols] = (dot(expo.astype(BF16), values) / total).astype(BF16)
            return 0

        lax.fori_loop(0, q_heads, one_head, 0)
        for which in range(2):
            place(
                ctx_stage.at[pl.ds(which * half, half)],
                lambda slot: ctx_out.at[pl.ds(pl.multiple_of(slot * half, half), half)],
                groups, block_id(which), which,
            )

    lag = 2 * n - 1
    last = pieces + lag
    attend_at = jnp.where(me == 0, lag, last)

    def slot_step(t, _):
        k_a = t - me
        k_b = t - (lag - me)

        @pl.when((k_a >= 0) & (k_a < pieces))
        def _():
            step_a(k_a)

        @pl.when(t == attend_at)
        def _():
            attention()

        @pl.when((k_b >= 0) & (k_b < pieces))
        def _():
            step_b(k_b)

        return 0

    lax.fori_loop(0, last + 1, slot_step, 0)

    def drain(k, _):
        @pl.when(me < n - 1)
        def _():
            remote(out_a.at[k], buf_a.at[k], a_send.at[k], a_recv.at[k], me).wait_send()

        @pl.when(me > 0)
        def _():
            remote(out_b.at[k], buf_b.at[k], b_send.at[k], b_recv.at[k], me).wait_send()

        return 0

    lax.fori_loop(0, pieces, drain, 0)

    def drain_kv(s, _):
        @pl.when(s > me)
        def _():
            for copy in kv_copies(s, s, me, first):
                copy.wait_send()

        @pl.when(s < me)
        def _():
            for copy in kv_copies(s, s, me, both):
                copy.wait_send()

        return 0

    lax.fori_loop(0, n, drain_kv, 0)

    for which in range(2):
        rows = pl.ds(which * half, half)
        for kind in range(groups + 1):
            if kind < groups:
                cols = pl.ds(kind * group_width, group_width)
                src, dst = mix_stage.at[rows, cols], mix_out.at[rows, cols]
            else:
                src, dst = ctx_stage.at[rows], ctx_out.at[rows]
            copy = remote(src, dst, o_send.at[kind, which], o_recv.at[kind, which], me)

            @pl.when(block_id(which) // 2 != me)
            def _():
                copy.wait_send()

            copy.wait_recv()


def body(n, query, keys, values, m_x, m_z, m_b, m_c, dt_raw, dt_bias, a_log, d_skip, norm_gain):
    tok, width = m_x.shape
    half = tok // 2
    heads = dt_raw.shape[1]
    groups = m_b.shape[1] // MN
    piece = math.gcd(width // groups, 256)
    pieces = width // piece
    kv = keys.shape[1]
    dma = pltpu.SemaphoreType.DMA
    vmem = pltpu.VMEM
    state = (pieces, MN, piece)
    spec = pl.BlockSpec(memory_space=pltpu.VMEM)
    return pl.pallas_call(
        functools.partial(kernel, n),
        out_shape=(
            jax.ShapeDtypeStruct(query.shape, BF16),
            jax.ShapeDtypeStruct(m_x.shape, BF16),
        ),
        in_specs=[spec] * 12,
        out_specs=(spec, spec),
        scratch_shapes=[
            vmem((n, tok, kv), BF16),
            vmem((n, tok, kv), BF16),
            vmem((tok, n * tok), F32),
            vmem(query.shape, BF16),
            vmem(m_x.shape, BF16),
            vmem(m_x.shape, BF16),
            vmem((half, width), F32),
            vmem((half, width), F32),
            vmem((2 * tok + 8, heads), F32),
            vmem((heads, tok), F32),
            vmem((groups, tok, tok), F32),
            vmem(state, BF16),
            vmem(state, BF16),
            vmem(state, BF16),
            vmem(state, BF16),
            vmem(state, F32),
            vmem((pieces, 8, piece), F32),
            dma((n,)),
            dma((n,)),
            dma((n,)),
            dma((n,)),
            dma((pieces,)),
            dma((pieces,)),
            dma((pieces,)),
            dma((pieces,)),
            dma((groups + 1, 2)),
            dma((groups + 1, 2)),
        ],
        compiler_params=pltpu.CompilerParams(
            collective_id=0, has_side_effects=True, vmem_limit_bytes=48 * 1024 * 1024
        ),
    )(
        query, keys, values, m_x, m_z, m_b, m_c, dt_raw,
        dt_bias.reshape(1, -1), a_log.reshape(1, -1), d_skip.reshape(1, -1), norm_gain.reshape(1, -1),
    )


def solution(mesh):
    rows = P(("grp", "ctx"), "hd")
    in_specs = (rows,) * 8 + (P("hd"),) * 4
    return jax.shard_map(
        functools.partial(body, mesh.shape["ctx"]),
        mesh=mesh, in_specs=in_specs, out_specs=(rows, rows), check_vma=False,
    )
```

```python
import functools
import math

import jax
import jax.numpy as jnp
from jax import lax
from jax.experimental import pallas as pl
from jax.experimental.pallas import tpu as pltpu
from jax.sharding import PartitionSpec as P

HEAD_SIZE = 128
MP = 64
MN = 128
NORM_EPS = 1e-05
MASKED = -1e30
HIGHEST = lax.Precision.HIGHEST
F32 = jnp.float32
BF16 = jnp.bfloat16
INPUT_SPACE = pltpu.HBM
HOP_SLOTS = 3
PIECE = 256


def dot(a, b, ca=1, cb=0, precision=None):
    return lax.dot_general(
        a, b, (((ca,), (cb,)), ((), ())), preferred_element_type=F32, precision=precision
    )


def kernel(
    n, q_in, k_ref, v_ref, x_in, z_in, b_in, c_in, dt_in, bias_in, alog_in, skip_in,
    gain_in, ctx_out, mix_out,
    q_ref, x_ref, z_ref, b_ref, c_ref, dt_ref, bias_ref, alog_ref, skip_ref, gain_ref,
    k_all, v_all, bias_scr, ctx_stage, arrived, gated, base_scr, er_scr, xdt_scr, hs, runt, gmask,
    buf_a, buf_b, out_a, out_b, sloc_a, sloc_b, tot_a, tot_b,
    k_send, k_recv, v_send, v_recv, a_send, a_recv, b_send, b_recv, o_send, o_recv, load_sem,
):
    me = lax.axis_index("ctx")
    tok = q_ref.shape[0]
    half = tok // 2
    heads = dt_ref.shape[0]
    width = x_ref.shape[1]
    groups = b_ref.shape[1] // MN
    group_width = width // groups
    pieces, _, piece = buf_a.shape
    per_piece = piece // MP
    per_group = group_width // piece
    q_heads = q_ref.shape[1] // HEAD_SIZE
    repeat = q_ref.shape[1] // k_ref.shape[1]
    mesh_id = pl.DeviceIdType.MESH

    loads = [
        pltpu.make_async_copy(src, dst, load_sem.at[i])
        for i, (src, dst) in enumerate(
            (
                (dt_in, dt_ref), (bias_in, bias_ref), (alog_in, alog_ref), (skip_in, skip_ref),
                (b_in, b_ref), (c_in, c_ref), (x_in, x_ref), (gain_in, gain_ref), (z_in, z_ref),
                (k_ref, k_all.at[me]), (v_ref, v_all.at[me]), (q_in, q_ref),
            )
        )
    ]
    for load in loads:
        load.start()

    barrier = pltpu.get_barrier_semaphore()

    def greet(d, _):
        peer = lax.rem(me + d, n)
        pl.semaphore_signal(barrier, inc=1, device_id={"ctx": peer}, device_id_type=mesh_id)
        return 0

    lax.fori_loop(1, n, greet, 0)
    pl.semaphore_wait(barrier, n - 1)

    def remote(src, dst, send, recv, peer):
        return pltpu.make_async_remote_copy(
            src_ref=src, dst_ref=dst, send_sem=send, recv_sem=recv,
            device_id={"ctx": peer}, device_id_type=mesh_id,
        )

    def kv_copies(slot, sem_slot, peer, rows):
        return (
            remote(k_ref.at[rows], k_all.at[slot, rows], k_send.at[sem_slot], k_recv.at[slot], peer),
            remote(v_ref.at[rows], v_all.at[slot, rows], v_send.at[sem_slot], v_recv.at[slot], peer),
        )

    first = pl.ds(0, half)
    both = pl.ds(0, tok)

    def start_kv(d, _):
        @pl.when(me + d < n)
        def _():
            for copy in kv_copies(me, me + d, me + d, first):
                copy.start()

        @pl.when(me - d >= 0)
        def _():
            for copy in kv_copies(me, me - d, me - d, both):
                copy.start()

        return 0

    lax.fori_loop(1, n, start_kv, 0)

    row = lax.broadcasted_iota(jnp.int32, (tok, tok), 0)
    col = lax.broadcasted_iota(jnp.int32, (tok, tok), 1)
    for load in loads[:4]:
        load.wait()
    raw = dot((row == col).astype(BF16), dt_ref[...], 1, 1) + bias_ref[...]
    steps = jnp.maximum(raw, 0.0) + jnp.log1p(jnp.exp(-jnp.abs(raw)))
    decay = -steps * jnp.exp(alog_ref[...])
    lower = (col <= row) & ((row < half) == (col < half))
    tri = lower.astype(F32)
    hs[0:tok, :] = dot(tri, decay, precision=HIGHEST)
    hs[tok : 2 * tok, :] = steps
    hs[2 * tok :, :] = jnp.broadcast_to(skip_ref[...], (8, heads))
    runt[...] = dot(decay, tri, 0, 1, precision=HIGHEST)
    for load in loads[4:6]:
        load.wait()
    for g in range(groups):
        cols = slice(g * MN, (g + 1) * MN)
        gmask[g] = jnp.where(lower, dot(c_ref[:, cols], b_ref[:, cols], 1, 1), 0.0)

    @pl.when(me == 0)
    def _():
        buf_a[...] = jnp.zeros_like(buf_a)

    lane_head = lax.broadcasted_iota(jnp.int32, (heads, piece), 1) // MP
    head_row = lax.broadcasted_iota(jnp.int32, (heads, piece), 0)
    wide_head = lax.broadcasted_iota(jnp.int32, (heads, per_piece * tok), 1) // tok
    wide_row = lax.broadcasted_iota(jnp.int32, (heads, per_piece * tok), 0)
    left = lax.broadcasted_iota(jnp.int32, (tok, 2 * MP), 1) < MP

    def place(src, dst_of, kind, block_id, which):
        owner = block_id // 2
        slot = lax.rem(block_id, 2)

        @pl.when(owner == me)
        def _():
            pltpu.make_async_copy(src, dst_of(slot), o_recv.at[kind, slot]).start()

        @pl.when(owner != me)
        def _():
            remote(src, dst_of(slot), o_send.at[kind, which], o_recv.at[kind, slot], owner).start()

    def block_id(which):
        return me if which == 0 else 2 * n - 1 - me

    def send_piece(k, which):
        cols = pl.ds(pl.multiple_of(k * piece, piece), piece)
        place(
            gated.at[pl.ds(which * half, half), cols],
            lambda slot: arrived.at[pl.ds(pl.multiple_of(slot * half, half), half), cols],
            k, block_id(which), which,
        )

    def silu(value):
        return value / (1.0 + jnp.exp(-value))

    def prepare(k):
        cols = pl.ds(pl.multiple_of(k * piece, piece), piece)
        gcols = pl.ds(pl.multiple_of((k // per_group) * MN, MN), MN)
        pick = (head_row == k * per_piece + lane_head).astype(F32)
        spread = dot(hs[...], pick, precision=HIGHEST)
        run, step, skip = spread[0:tok], spread[tok : 2 * tok], spread[2 * tok : 2 * tok + 1]
        xs = x_ref[:, cols].astype(F32)
        xdt = xs * step
        last_a, last_b = run[half - 1 : half], run[tok - 1 : tok]
        b_rows = b_ref[:, gcols]
        sloc_a[k] = dot(b_rows[0:half], (xdt[0:half] * jnp.exp(last_a - run[0:half])).astype(BF16), 0, 0)
        sloc_b[k] = dot(b_rows[half:], (xdt[half:] * jnp.exp(last_b - run[half:])).astype(BF16), 0, 0)
        tot_a[k] = jnp.broadcast_to(jnp.exp(last_a), (8, piece))
        tot_b[k] = jnp.broadcast_to(jnp.exp(last_b), (8, piece))
        er_scr[:, cols] = jnp.exp(run)
        xdt_scr[:, cols] = xdt.astype(BF16)
        base_scr[:, cols] = skip * xs

    def within_blocks(k, _):
        cols = pl.ds(pl.multiple_of(k * piece, piece), piece)
        wide = dot(hs[0:tok, :], (wide_row == k * per_piece + wide_head).astype(F32), precision=HIGHEST)
        gm = gmask[k // per_group]
        inner = []
        for pair in range(per_piece // 2):
            weights = []
            for which in range(2):
                h = 2 * pair + which
                gap = wide[:, h * tok : (h + 1) * tok] - runt[pl.ds(k * per_piece + h, 1), :]
                weights.append((jnp.exp(jnp.minimum(gap, 0.0)) * gm).astype(BF16))
            at = pl.ds(pl.multiple_of(k * piece + pair * 2 * MP, 2 * MP), 2 * MP)
            part = xdt_scr[:, at]
            none = jnp.zeros_like(part)
            stacked = jnp.concatenate([jnp.where(left, part, none), jnp.where(left, none, part)], axis=0)
            inner.append(dot(jnp.concatenate(weights, axis=1), stacked))
        base_scr[:, cols] = base_scr[:, cols] + jnp.concatenate(inner, axis=1)
        return 0

    def gate(k, which, buffer):
        cols = pl.ds(pl.multiple_of(k * piece, piece), piece)
        gcols = pl.ds(pl.multiple_of((k // per_group) * MN, MN), MN)
        rows = slice(which * half, (which + 1) * half)
        carried = dot(c_ref[rows, gcols], buffer[k]) * er_scr[rows, cols]
        z = z_ref[rows, cols].astype(F32)
        gated[rows, cols] = ((base_scr[rows, cols] + carried) * silu(z)).astype(BF16)
        send_piece(k, which)

    def gate_a(k, _):
        gate(k, 0, buf_a)
        return 0

    def step_a(k):
        @pl.when(me == 0)
        def _():
            prepare(k)

        @pl.when(me > 0)
        def _():
            remote(out_a.at[k], buf_a.at[k], a_send.at[k], a_recv.at[k], me).wait_recv()

        state = (buf_a[k].astype(F32) * tot_a[k][0:1] + sloc_a[k]).astype(BF16)

        @pl.when(me < n - 1)
        def _():
            out_a[k] = state
            remote(out_a.at[k], buf_a.at[k], a_send.at[k], a_recv.at[k], me + 1).start()

        @pl.when(me == n - 1)
        def _():
            buf_b[k] = state

    def step_b(k):
        @pl.when(me < n - 1)
        def _():
            remote(out_b.at[k], buf_b.at[k], b_send.at[k], b_recv.at[k], me).wait_recv()

        @pl.when(me > 0)
        def _():
            out_b[k] = (buf_b[k].astype(F32) * tot_b[k][0:1] + sloc_b[k]).astype(BF16)
            remote(out_b.at[k], buf_b.at[k], b_send.at[k], b_recv.at[k], me - 1).start()

        gate(k, 1, buf_b)

    def attention():
        def wait_kv(s, _):
            @pl.when(s < me)
            def _():
                for copy in kv_copies(s, s, me, first):
                    copy.wait_recv()
                k_all[s, half:, :] = jnp.zeros((half, k_ref.shape[1]), BF16)
                v_all[s, half:, :] = jnp.zeros((half, k_ref.shape[1]), BF16)

            @pl.when(s > me)
            def _():
                for copy in kv_copies(s, s, me, both):
                    copy.wait_recv()

            return 0

        lax.fori_loop(0, n, wait_kv, 0)
        for load in loads[9:]:
            load.wait()
        key = lax.broadcasted_iota(jnp.int32, (tok, n * tok), 1)
        source = key // tok
        within = key - source * tok
        key_pos = jnp.where(
            within < half, source * half + within, (2 * n - 2 - source) * half + within
        )
        query = lax.broadcasted_iota(jnp.int32, (tok, n * tok), 0)
        query_pos = jnp.where(query < half, me * half + query, (2 * n - 2 - me) * half + query)
        bias_scr[...] = jnp.where(key_pos <= query_pos, 0.0, MASKED)
        scale = 1.0 / math.sqrt(HEAD_SIZE)

        def one_head(h, _):
            hcols = pl.ds(pl.multiple_of(h * HEAD_SIZE, HEAD_SIZE), HEAD_SIZE)
            kcols = pl.ds(pl.multiple_of((h // repeat) * HEAD_SIZE, HEAD_SIZE), HEAD_SIZE)
            keys = k_all[:, :, kcols].reshape(n * tok, HEAD_SIZE)
            values = v_all[:, :, kcols].reshape(n * tok, HEAD_SIZE)
            scores = dot(q_ref[:, hcols], keys, 1, 1) * scale + bias_scr[...]
            expo = jnp.exp(scores - jnp.max(scores, axis=-1, keepdims=True))
            total = jnp.sum(expo, axis=-1, keepdims=True)
            ctx_stage[:, hcols] = (dot(expo.astype(BF16), values) / total).astype(BF16)
            return 0

        lax.fori_loop(0, q_heads, one_head, 0)
        for which in range(2):
            place(
                ctx_stage.at[pl.ds(which * half, half)],
                lambda slot: ctx_out.at[pl.ds(pl.multiple_of(slot * half, half), half)],
                pieces, block_id(which), which,
            )

    for load in loads[6:9]:
        load.wait()
    lag = 2 * (n - 1) * HOP_SLOTS
    last = pieces + lag
    b_start = lag - me * HOP_SLOTS
    idle_between = me * HOP_SLOTS + pieces <= b_start
    attend_at = jnp.where(idle_between, b_start, last)

    def prepare_early(k, _):
        prepare(k)
        return 0

    @pl.when(me > 0)
    def _():
        lax.fori_loop(0, pieces, prepare_early, 0)

    inner_at = jnp.where(idle_between, b_start, 0)

    def slot_step(t, _):
        k_a = t - me * HOP_SLOTS
        k_b = t - (lag - me * HOP_SLOTS)

        @pl.when(t == inner_at)
        def _():
            lax.fori_loop(0, pieces, within_blocks, 0)

        @pl.when((k_a >= 0) & (k_a < pieces))
        def _():
            step_a(k_a)

        @pl.when(t == attend_at)
        def _():
            attention()
            lax.fori_loop(0, pieces, gate_a, 0)

        @pl.when((k_b >= 0) & (k_b < pieces))
        def _():
            step_b(k_b)

        return 0

    lax.fori_loop(0, last + 1, slot_step, 0)

    def drain(k, _):
        @pl.when(me < n - 1)
        def _():
            remote(out_a.at[k], buf_a.at[k], a_send.at[k], a_recv.at[k], me).wait_send()

        @pl.when(me > 0)
        def _():
            remote(out_b.at[k], buf_b.at[k], b_send.at[k], b_recv.at[k], me).wait_send()

        return 0

    lax.fori_loop(0, pieces, drain, 0)

    def drain_kv(s, _):
        @pl.when(s > me)
        def _():
            for copy in kv_copies(s, s, me, first):
                copy.wait_send()

        @pl.when(s < me)
        def _():
            for copy in kv_copies(s, s, me, both):
                copy.wait_send()

        return 0

    lax.fori_loop(0, n, drain_kv, 0)

    def await_placed(kind, which, src, dst):
        copy = remote(src, dst, o_send.at[kind, which], o_recv.at[kind, which], me)

        @pl.when(block_id(which) // 2 != me)
        def _():
            copy.wait_send()

        copy.wait_recv()

    for which in range(2):
        rows = pl.ds(which * half, half)
        await_placed(pieces, which, ctx_stage.at[rows], ctx_out.at[rows])
    for g in range(groups):
        gcols = slice(g * group_width, (g + 1) * group_width)
        for which in range(2):
            rows = pl.ds(which * half, half)
            for k in range(g * per_group, (g + 1) * per_group):
                cols = pl.ds(k * piece, piece)
                await_placed(k, which, gated.at[rows, cols], arrived.at[rows, cols])
            value = arrived[rows, gcols].astype(F32)
            power = jnp.mean(value * value, axis=-1, keepdims=True)
            mix_out[rows, gcols] = (value * lax.rsqrt(power + NORM_EPS) * gain_ref[:, gcols]).astype(BF16)


def body(n, query, keys, values, m_x, m_z, m_b, m_c, dt_raw, dt_bias, a_log, d_skip, norm_gain):
    tok, width = m_x.shape
    half = tok // 2
    heads = dt_raw.shape[1]
    anywhere = pl.BlockSpec(memory_space=INPUT_SPACE)
    groups = m_b.shape[1] // MN
    piece = math.gcd(width // groups, PIECE)
    pieces = width // piece
    kv = keys.shape[1]
    dma = pltpu.SemaphoreType.DMA
    vmem = pltpu.VMEM
    state = (pieces, MN, piece)
    spec = pl.BlockSpec(memory_space=pltpu.VMEM)
    return pl.pallas_call(
        functools.partial(kernel, n),
        out_shape=(
            jax.ShapeDtypeStruct(query.shape, BF16),
            jax.ShapeDtypeStruct(m_x.shape, BF16),
        ),
        in_specs=[anywhere] * 12,
        out_specs=(spec, spec),
        scratch_shapes=[
            vmem(query.shape, BF16),
            vmem(m_x.shape, BF16),
            vmem(m_x.shape, BF16),
            vmem(m_b.shape, BF16),
            vmem(m_b.shape, BF16),
            vmem((heads, tok), BF16),
            vmem((1, heads), F32),
            vmem((1, heads), F32),
            vmem((1, heads), F32),
            vmem((1, width), F32),
            vmem((n, tok, kv), BF16),
            vmem((n, tok, kv), BF16),
            vmem((tok, n * tok), F32),
            vmem(query.shape, BF16),
            vmem(m_x.shape, BF16),
            vmem(m_x.shape, BF16),
            vmem((tok, width), F32),
            vmem((tok, width), F32),
            vmem((tok, width), BF16),
            vmem((2 * tok + 8, heads), F32),
            vmem((heads, tok), F32),
            vmem((groups, tok, tok), F32),
            vmem(state, BF16),
            vmem(state, BF16),
            vmem(state, BF16),
            vmem(state, BF16),
            vmem(state, F32),
            vmem(state, F32),
            vmem((pieces, 8, piece), F32),
            vmem((pieces, 8, piece), F32),
            dma((n,)),
            dma((n,)),
            dma((n,)),
            dma((n,)),
            dma((pieces,)),
            dma((pieces,)),
            dma((pieces,)),
            dma((pieces,)),
            dma((pieces + 1, 2)),
            dma((pieces + 1, 2)),
            dma((12,)),
        ],
        compiler_params=pltpu.CompilerParams(
            collective_id=0, has_side_effects=True, vmem_limit_bytes=67043328
        ),
    )(
        query, keys, values, m_x, m_z, m_b, m_c, dt_raw.T,
        dt_bias.reshape(1, -1), a_log.reshape(1, -1), d_skip.reshape(1, -1), norm_gain.reshape(1, -1),
    )


def solution(mesh):
    rows = P(("grp", "ctx"), "hd")
    in_specs = (rows,) * 8 + (P("hd"),) * 4
    return jax.shard_map(
        functools.partial(body, mesh.shape["ctx"]),
        mesh=mesh, in_specs=in_specs, out_specs=(rows, rows), check_vma=False,
    )
```
